32 devices in a mesh: seq: 4 (over z), head: 4 (over y, x), batch: 2 (over core).
Axes of the slice: x: 2, y: 2, z: 4, core: 2. Of those that a mesh axis runs over, the one named last changes fastest.
Arguments:
- ssm_input: bfloat16 [16384, 5120], P(('batch', 'seq'), 'head'), parts along dimension 0, may hold values from -500 to 500
- gate_input: bfloat16 [16384, 5120], P(('batch', 'seq'), 'head'), parts along dimension 0, may hold values from -6 to 6
- b_proj: bfloat16 [16384, 1024], P(('batch', 'seq')), parts along dimension 0, may hold values from -2 to 2
- c_proj: bfloat16 [16384, 1024], P(('batch', 'seq')), parts along dimension 0, may hold values from -2 to 2
- step_size: float32 [80, 16384], P('head', ('batch', 'seq')), parts along dimension 1, may hold values from 0.02 to 0.2
- log_decay: float32 [80, 16384], P('head', ('batch', 'seq')), parts along dimension 1, may hold values from -1.5 to 0, as said below
- skip_gain: float32 [80], P('head'), may hold values from 0.5 to 1.5
- norm_gain: float32 [5120], replicated, may hold values from 0.1 to 1.9
- out_weight: bfloat16 [5120, 2560], P('head'), may hold values from -0.078125 to 0.078125
Outputs:
- layer_out: bfloat16 [16384, 2560], P(('batch', 'seq', 'head')), parts along dimension 0
The draws below stay inside these ranges and needn't reach their ends.
There are 2 independent parts, one for each index of `batch`. The reference program is written for one: setup_inputs(seed, part) draws one part's arguments, and reference() takes and returns one part's arrays. A program takes and returns all parts, laid end to end along the dimension named above; an argument that names none is the same for every part. Nothing has to cross between parts.
Inputs may be any that keep to these rules, and one draw needn't show every extreme that they name: `log_decay`: negative.
All inputs are finite; a program needn't handle non-finite values.
Results may differ from the reference program's by a relative error of at most 0.018.
Values may be sent and summed in bfloat16 or wider, within the bound.
A program may use at most 192 MiB of HBM per device.

```python
import math
import jax
import jax.numpy as jnp
from jax import lax

D = 2560
HEAD_COUNT = 80
HEAD_DIM = 64
STATE = 128
GROUPS = 8
BLOCK = 256
SEQUENCE_LENGTH = 8192


def draw_ssm_input(key, part):
    random_keys = jax.random.split(key, 3)
    total_width = HEAD_COUNT * HEAD_DIM
    columns = 10.0 ** (jnp.arange(total_width, dtype=jnp.float32) / total_width)
    row_scale = 10.0 ** jax.random.uniform(random_keys[0], (SEQUENCE_LENGTH, 1), jnp.float32)
    values = jnp.clip(jax.random.normal(random_keys[2], (SEQUENCE_LENGTH, total_width), jnp.float32), -4.0, 4.0)
    return (values * columns[None, :] * row_scale).astype(jnp.bfloat16)


def draw_log_decay(key, part):
    random_keys = jax.random.split(key, 6)
    fast_share = 0.5
    is_fast = jax.random.uniform(random_keys[0], (HEAD_COUNT, 1), jnp.float32) < fast_share
    fast_rate = 10.0 ** jax.random.uniform(random_keys[1], (HEAD_COUNT, 1), jnp.float32, -1.699, -1.347)
    slow_rate = 10.0 ** jax.random.uniform(random_keys[2], (HEAD_COUNT, 1), jnp.float32, -1.0, 0.0) / SEQUENCE_LENGTH
    per_head_decay = jnp.where(is_fast, fast_rate, slow_rate)
    jitter_level = jax.random.uniform(random_keys[3], (HEAD_COUNT, SEQUENCE_LENGTH), jnp.float32, 0.2, 1.6)
    spike_position = jax.random.randint(random_keys[4], (2, 1), 0, SEQUENCE_LENGTH)
    spike_decay = jax.random.uniform(random_keys[5], (HEAD_COUNT, 2), jnp.float32, 0.22, 0.69)
    spike_count = (jnp.arange(SEQUENCE_LENGTH)[None, :] == spike_position).astype(jnp.float32)
    return -per_head_decay * jitter_level - jnp.dot(spike_decay, spike_count)


def shard_levels(key, dims, shards, smallest, high):
    def one(dim, shards_of):
        steps = jax.random.uniform(jax.random.fold_in(jax.random.fold_in(key, 6), dim), (shards_of,), jnp.float32, smallest / len(shards), high / len(shards))
        return jnp.repeat(jnp.exp(steps), dims[dim] // shards_of).reshape((-1,) + (1,) * (len(dims) - dim - 1))

    loudness = one(*shards[0])
    for cut in shards[1:]:
        loudness = loudness * one(*cut)
    return loudness


def gaussian(key, dims, deviation, bound, shards=(), held_as=jnp.bfloat16):
    drawn = jax.random.normal(key, dims, jnp.float32) * deviation
    if len(shards) > 0:
        drawn = shard_levels(key, dims, shards, -0.22, 0.18) * drawn
    return jnp.clip(drawn, min=-bound, max=bound).astype(held_as)


def setup_inputs(seed: int = 0, part: int = 0) -> dict:
    key_list = jax.random.split(jax.random.key(seed), 10)
    part_keys = jax.random.split(jax.random.fold_in(key_list[9], part), 10)
    return {
        "ssm_input": draw_ssm_input(jax.random.fold_in(jax.random.fold_in(key_list[9], part), 71), part),
        "gate_input": gaussian(part_keys[1], (SEQUENCE_LENGTH, HEAD_COUNT * HEAD_DIM), 1.5, 6.0, ((0, 4), (1, 4))),
        "b_proj": gaussian(part_keys[2], (SEQUENCE_LENGTH, GROUPS * STATE), 0.3, 2.0, ((0, 4),)),
        "c_proj": gaussian(part_keys[3], (SEQUENCE_LENGTH, GROUPS * STATE), 0.3, 2.0, ((0, 4),)),
        "step_size": jnp.clip(jnp.exp(math.log(0.2) - 2.3025851 * jax.random.uniform(part_keys[4], (HEAD_COUNT, SEQUENCE_LENGTH), jnp.float32) ** shard_levels(part_keys[4], (HEAD_COUNT, SEQUENCE_LENGTH), ((0, 4), (1, 4)), -0.2, 0.2)), 0.02, 0.2),
        "log_decay": draw_log_decay(jax.random.fold_in(jax.random.fold_in(key_list[9], part), 71), part),
        "skip_gain": jnp.clip(0.5 + 1.0 * jax.random.uniform(key_list[6], (HEAD_COUNT,), jnp.float32) ** shard_levels(key_list[6], (HEAD_COUNT,), ((0, 4),), -0.2, 0.2), 0.5, 1.5),
        "norm_gain": jnp.clip(1.0 + 0.18 * jax.random.normal(key_list[7], (HEAD_COUNT * HEAD_DIM,), jnp.float32), 0.1, 1.9),
        "out_weight": gaussian(key_list[8], (HEAD_COUNT * HEAD_DIM, D), (HEAD_COUNT * HEAD_DIM) ** -0.5, 0.078125, ((0, 4),)),
    }


epsilon = 1e-05

def reference(ssm_input, gate_input, b_proj, c_proj, step_size, log_decay, skip_gain, norm_gain, out_weight):
    nblocks = SEQUENCE_LENGTH // BLOCK
    group_of = jnp.arange(HEAD_COUNT) // (HEAD_COUNT // GROUPS)
    lower_mask = jnp.tril(jnp.ones((BLOCK, BLOCK), dtype=bool))

    def block_step(carried, inputs_now):
        x_block, b_block, c_block, step_block, decay_block = inputs_now
        cumulative = jnp.cumsum(decay_block, axis=1)
        b_heads = b_block.reshape(BLOCK, GROUPS, STATE)[:, group_of, :].astype(jnp.float32)
        c_heads = c_block.reshape(BLOCK, GROUPS, STATE)[:, group_of, :].astype(jnp.float32)
        scores = jnp.einsum('thn,shn->hts', c_heads, b_heads)
        differ = cumulative[:, :, None] - cumulative[:, None, :]
        weights = scores * jnp.exp(jnp.where(lower_mask, differ, -jnp.inf)) * step_block[:, None, :]
        weights = lax.optimization_barrier(weights.astype(jnp.bfloat16)).astype(jnp.float32)
        x_heads = x_block.reshape(BLOCK, HEAD_COUNT, HEAD_DIM).astype(jnp.float32)
        within = jnp.einsum('hts,shp->thp', weights, x_heads)
        entering_b = lax.optimization_barrier(carried.astype(jnp.bfloat16)).astype(jnp.float32)
        across = jnp.einsum('thn,hpn->thp', c_heads, entering_b) * jnp.exp(cumulative).T[:, :, None]
        to_end = (jnp.exp(cumulative[:, -1:] - cumulative) * step_block).T
        scaled = lax.optimization_barrier((b_heads * to_end[:, :, None]).astype(jnp.bfloat16)).astype(jnp.float32)
        block_state = jnp.einsum('shp,shn->hpn', x_heads, scaled)
        renewed = jnp.exp(cumulative[:, -1])[:, None, None] * carried + block_state
        output = within + across + skip_gain[None, :, None] * x_heads
        return (renewed, output)
    x_blocks = ssm_input.reshape(nblocks, BLOCK, HEAD_COUNT * HEAD_DIM)
    b_blocks = b_proj.reshape(nblocks, BLOCK, GROUPS * STATE)
    c_blocks = c_proj.reshape(nblocks, BLOCK, GROUPS * STATE)
    step_blocks = step_size.reshape(HEAD_COUNT, nblocks, BLOCK).transpose(1, 0, 2)
    decay_blocks = log_decay.reshape(HEAD_COUNT, nblocks, BLOCK).transpose(1, 0, 2)
    start_state = jnp.zeros((HEAD_COUNT, HEAD_DIM, STATE), jnp.float32)
    unused, outputs = lax.scan(block_step, start_state, (x_blocks, b_blocks, c_blocks, step_blocks, decay_blocks))
    output = outputs.reshape(SEQUENCE_LENGTH, HEAD_COUNT * HEAD_DIM)
    gated_rows = output * jax.nn.silu(gate_input.astype(jnp.float32))
    squares = lax.optimization_barrier(jnp.sum(gated_rows * gated_rows, axis=1, keepdims=True))
    normed = (gated_rows * lax.rsqrt(squares / (HEAD_COUNT * HEAD_DIM) + epsilon) * norm_gain).astype(jnp.bfloat16)
    return jnp.dot(normed, out_weight, preferred_element_type=jnp.float32).astype(jnp.bfloat16)
```

```python
import functools
import jax
import jax.numpy as jnp
from jax import lax
from jax.experimental import pallas as pl
from jax.experimental.pallas import tpu as pltpu
from jax.sharding import PartitionSpec as P

HEAD_COUNT = 80
HEAD_DIM = 64
STATE = 128
GROUPS = 8
BLOCK = 256
LANES = 128
epsilon = 1e-05
HIGHEST = lax.Precision.HIGHEST
F32 = jnp.float32
BF16 = jnp.bfloat16


def dot(a, b, ca, cb, precision=None):
    return lax.dot_general(
        a, b, (((ca,), (cb,)), ((), ())), precision=precision, preferred_element_type=F32
    )


def iotas(rows, columns):
    return (
        lax.broadcasted_iota(jnp.int32, (rows, columns), 0),
        lax.broadcasted_iota(jnp.int32, (rows, columns), 1),
    )


def lower_ones():
    t, s = iotas(BLOCK, BLOCK)
    return jnp.where(s <= t, 1.0, 0.0).astype(F32)


def identity():
    t, s = iotas(BLOCK, BLOCK)
    return jnp.where(s == t, 1.0, 0.0).astype(F32)


def pieces(channels, repeats):
    found = []
    for start in range(0, channels, LANES):
        width = min(LANES, channels - start)
        heads = [start // HEAD_DIM + i for i in range(width // HEAD_DIM)]
        found.append((start, width, heads, heads[0] // repeats))
    return found


def spread(columns, heads, width):
    first = jnp.broadcast_to(columns[:, heads[0] : heads[0] + 1], (BLOCK, width))
    if len(heads) == 1:
        return first
    second = jnp.broadcast_to(columns[:, heads[1] : heads[1] + 1], (BLOCK, width))
    lane = iotas(BLOCK, width)[1]
    return jnp.where(lane < HEAD_DIM, first, second)


def state_kernel(
    repeats, at_ref, x_ref, b_ref, step_ref, log_ref, prefix_ref, base_ref, total_ref, all_ref, s_ref, l_ref
):
    k = pl.program_id(0)
    channels = x_ref.shape[1]

    @pl.when(k == 0)
    def _():
        s_ref[...] = jnp.zeros_like(s_ref)
        l_ref[...] = jnp.zeros_like(l_ref)

    columns = dot(lower_ones(), log_ref[...], 1, 1, HIGHEST)
    steps = dot(identity(), step_ref[...], 1, 1, HIGHEST)
    base_ref[0] = l_ref[...]
    prefix_ref[0] = s_ref[...].astype(BF16)
    for start, width, heads, group in pieces(channels, repeats):
        lanes = pl.ds(start, width)
        cum = spread(columns, heads, width)
        last = cum[BLOCK - 1 : BLOCK, :]
        weighted = (
            x_ref[:, lanes].astype(F32) * (jnp.exp(last - cum) * spread(steps, heads, width))
        ).astype(BF16)
        new = dot(b_ref[:, group * STATE : (group + 1) * STATE], weighted, 0, 0)
        s_ref[:, lanes] = jnp.exp(last) * s_ref[:, lanes] + new
        l_ref[:, lanes] = l_ref[:, lanes] + last
    total_ref[...] = s_ref[...]
    all_ref[...] = jnp.exp(l_ref[...])


def within_kernel(
    repeats, at_ref, x_ref, b_ref, c_ref, step_ref, log_ref, skip_ref, prefix_ref, y_ref
):
    channels = x_ref.shape[1]
    half = BLOCK // 2
    lower = lower_ones()
    columns = dot(lower, log_ref[...], 1, 1, HIGHEST)
    rows = dot(log_ref[...], lower, 1, 1, HIGHEST) - jnp.log(step_ref[...])
    scores = {}
    for start, width, heads, group in pieces(channels, repeats):
        lanes = pl.ds(start, width)
        c_here = c_ref[:, group * STATE : (group + 1) * STATE]
        if group not in scores:
            full = dot(c_here, b_ref[:, group * STATE : (group + 1) * STATE], 1, 1)
            scores[group] = full * lower
        x_here = x_ref[:, lanes]
        lane = iotas(BLOCK, width)[1]
        top, bottom = 0.0, 0.0
        for i, head in enumerate(heads):
            kept = (lane >= i * HEAD_DIM) & (lane < (i + 1) * HEAD_DIM)
            x_head = x_here if len(heads) == 1 else jnp.where(kept, x_here, jnp.zeros_like(x_here))
            column, row = columns[:, head : head + 1], rows[head : head + 1, :]
            w_top = scores[group][:half, :half] * jnp.exp(
                jnp.minimum(column[:half] - row[:, :half], 0.0)
            )
            w_bottom = scores[group][half:] * jnp.exp(jnp.minimum(column[half:] - row, 0.0))
            top = top + dot(w_top.astype(BF16), x_head[:half], 1, 0)
            bottom = bottom + dot(w_bottom.astype(BF16), x_head, 1, 0)
        across = jnp.exp(spread(columns, heads, width)) * dot(c_here, prefix_ref[0, :, lanes], 1, 0)
        rest = across + skip_ref[:, lanes] * x_here.astype(F32)
        y_ref[:half, lanes] = (top + rest[:half]).astype(BF16)
        y_ref[half:, lanes] = (bottom + rest[half:]).astype(BF16)


def finish_kernel(
    repeats, at_ref, y_ref, gate_ref, c_ref, log_ref, base_ref, in_ref, gain_ref, w_ref, out_ref, sq_ref, g_ref
):
    channels = y_ref.shape[1]
    columns = dot(lower_ones(), log_ref[...], 1, 1, HIGHEST)
    squares = jnp.zeros((8, BLOCK), F32)
    for start, width, heads, group in pieces(channels, repeats):
        lanes = pl.ds(start, width)
        grow = jnp.exp(spread(columns, heads, width) + base_ref[0, 0:1, lanes])
        across = grow * dot(c_ref[:, group * STATE : (group + 1) * STATE], in_ref[:, lanes], 1, 0)
        gate = gate_ref[:, lanes].astype(F32)
        gated = (y_ref[:, lanes].astype(F32) + across) * (gate / (1.0 + jnp.exp(-gate)))
        squares = squares + dot(jnp.ones((8, width), BF16), (gated * gated).astype(BF16), 1, 1)
        g_ref[:, lanes] = (gated * gain_ref[:, lanes]).astype(BF16)
    sq_ref[...] = squares
    model = w_ref.shape[1]
    tile = 512 if model % 512 == 0 else model
    for start in range(0, model, tile):
        out_ref[:, start : start + tile] = dot(
            g_ref[...], w_ref[:, start : start + tile], 1, 0
        ).astype(BF16)


def shifted(value, axis, steps):
    count = lax.axis_size(axis)
    return lax.ppermute(value, axis, [(source, source + steps) for source in range(count - steps)])


def body(
    ssm_input, gate_input, b_proj, c_proj, step_size, log_decay, skip_gain, norm_gain, out_weight
):
    tokens, channels = ssm_input.shape
    heads = step_size.shape[0]
    blocks = tokens // BLOCK
    model = out_weight.shape[1]
    per_group = HEAD_COUNT // GROUPS
    groups = max(1, heads // per_group)
    repeats = min(heads, per_group)
    head_index = lax.axis_index("head")
    at = (head_index * heads // per_group // groups).astype(jnp.int32).reshape(1)
    skip = jnp.repeat(skip_gain, HEAD_DIM)[None, :]
    gain = lax.dynamic_slice_in_dim(norm_gain, head_index * channels, channels)[None, :]
    params = pltpu.CompilerParams(
        dimension_semantics=("arbitrary",), vmem_limit_bytes=56 * 1024 * 1024
    )

    def rows_of(width):
        return pl.BlockSpec((BLOCK, width), lambda k, at: (k, 0))

    grouped = pl.BlockSpec((BLOCK, groups * STATE), lambda k, at: (k, at[0]))
    head_rows = pl.BlockSpec((heads, BLOCK), lambda k, at: (0, k))
    fixed = lambda r, c: pl.BlockSpec((r, c), lambda k, at: (0, 0))
    state_block = pl.BlockSpec((1, STATE, channels), lambda k, at: (k, 0, 0))

    prefix, base, total, decay = pl.pallas_call(
        functools.partial(state_kernel, repeats),
        grid_spec=pltpu.PrefetchScalarGridSpec(
            num_scalar_prefetch=1,
            grid=(blocks,),
            in_specs=[rows_of(channels), grouped, head_rows, head_rows],
            out_specs=[
                state_block,
                pl.BlockSpec((1, 8, channels), lambda k, at: (k, 0, 0)),
                fixed(STATE, channels),
                fixed(8, channels),
            ],
            scratch_shapes=[pltpu.VMEM((STATE, channels), F32), pltpu.VMEM((8, channels), F32)],
        ),
        out_shape=[
            jax.ShapeDtypeStruct((blocks, STATE, channels), BF16),
            jax.ShapeDtypeStruct((blocks, 8, channels), F32),
            jax.ShapeDtypeStruct((STATE, channels), F32),
            jax.ShapeDtypeStruct((8, channels), F32),
        ],
        compiler_params=params,
        name="block_states",
        cost_estimate=pl.CostEstimate(
            flops=2 * tokens * channels * STATE, bytes_accessed=tokens * channels * 4, transcendentals=0
        ),
    )(at, ssm_input, b_proj, step_size, log_decay)

    incoming = shifted(total.astype(BF16), "seq", 1)
    for _ in range(lax.axis_size("seq") - 2):
        incoming = shifted((decay[0:1] * incoming.astype(F32) + total).astype(BF16), "seq", 1)

    y = pl.pallas_call(
        functools.partial(within_kernel, repeats),
        grid_spec=pltpu.PrefetchScalarGridSpec(
            num_scalar_prefetch=1,
            grid=(blocks,),
            in_specs=[
                rows_of(channels),
                grouped,
                grouped,
                head_rows,
                head_rows,
                fixed(1, channels),
                state_block,
            ],
            out_specs=rows_of(channels),
        ),
        out_shape=jax.ShapeDtypeStruct((tokens, channels), BF16),
        compiler_params=params,
        name="within",
        cost_estimate=pl.CostEstimate(
            flops=16 * tokens * channels * BLOCK, bytes_accessed=tokens * channels * 8, transcendentals=0
        ),
    )(at, ssm_input, b_proj, c_proj, step_size, log_decay, skip, prefix)

    shares = lax.axis_size("head")
    per_share = tokens // shares
    chunks = max(1, per_share // BLOCK)
    steps = blocks // chunks
    parts, squares = [], []
    for chunk in range(chunks):
        pick = lambda d, chunk=chunk: d * chunks + chunk
        partial, square = pl.pallas_call(
            functools.partial(finish_kernel, repeats),
            grid_spec=pltpu.PrefetchScalarGridSpec(
                num_scalar_prefetch=1,
                grid=(steps,),
                in_specs=[
                    pl.BlockSpec((BLOCK, channels), lambda d, at: (pick(d), 0)),
                    pl.BlockSpec((BLOCK, channels), lambda d, at: (pick(d), 0)),
                    pl.BlockSpec((BLOCK, groups * STATE), lambda d, at: (pick(d), at[0])),
                    pl.BlockSpec((heads, BLOCK), lambda d, at: (0, pick(d))),
                    pl.BlockSpec((1, 8, channels), lambda d, at: (pick(d), 0, 0)),
                    fixed(STATE, channels),
                    fixed(1, channels),
                    fixed(channels, model),
                ],
                out_specs=[
                    pl.BlockSpec((BLOCK, model), lambda d, at: (d, 0)),
                    pl.BlockSpec((8, BLOCK), lambda d, at: (0, d)),
                ],
                scratch_shapes=[pltpu.VMEM((BLOCK, channels), BF16)],
            ),
            out_shape=[
                jax.ShapeDtypeStruct((steps * BLOCK, model), BF16),
                jax.ShapeDtypeStruct((8, steps * BLOCK), F32),
            ],
            compiler_params=params,
            name="finish",
            cost_estimate=pl.CostEstimate(
                flops=2 * steps * BLOCK * channels * model,
                bytes_accessed=steps * BLOCK * (channels * 4 + model * 2) + channels * model * 2,
                transcendentals=0,
            ),
        )(at, y, gate_input, c_proj, log_decay, base, incoming, gain, out_weight)
        parts.append(lax.psum_scatter(partial, "head", scatter_dimension=0, tiled=True))
        squares.append(square[0].reshape(shares, per_share // chunks))
    squares = lax.psum_scatter(
        jnp.concatenate(squares, axis=1), "head", scatter_dimension=0, tiled=True
    ).reshape(per_share, 1)
    scale = lax.rsqrt(squares / (HEAD_COUNT * HEAD_DIM) + epsilon)
    return (jnp.concatenate(parts, axis=0).astype(F32) * scale).astype(BF16)


def solution(mesh):
    in_specs = (
        P(("batch", "seq"), "head"),
        P(("batch", "seq"), "head"),
        P(("batch", "seq"), None),
        P(("batch", "seq"), None),
        P("head", ("batch", "seq")),
        P("head", ("batch", "seq")),
        P("head"),
        P(),
        P("head", None),
    )
    out_specs = P(("batch", "seq", "head"), None)
    return jax.shard_map(body, mesh=mesh, in_specs=in_specs, out_specs=out_specs, check_vma=False)
```

```python
import functools
import jax
import jax.numpy as jnp
from jax import lax
from jax.experimental import pallas as pl
from jax.experimental.pallas import tpu as pltpu
from jax.sharding import PartitionSpec as P

HEAD_COUNT = 80
HEAD_DIM = 64
STATE = 128
GROUPS = 8
BLOCK = 256
LANES = 128
epsilon = 1e-05
HIGHEST = lax.Precision.HIGHEST
F32 = jnp.float32
BF16 = jnp.bfloat16


def dot(a, b, ca, cb, precision=None):
    return lax.dot_general(
        a, b, (((ca,), (cb,)), ((), ())), precision=precision, preferred_element_type=F32
    )


def iotas(rows, columns):
    return (
        lax.broadcasted_iota(jnp.int32, (rows, columns), 0),
        lax.broadcasted_iota(jnp.int32, (rows, columns), 1),
    )


def lower_ones():
    t, s = iotas(BLOCK, BLOCK)
    return jnp.where(s <= t, 1.0, 0.0).astype(F32)


def identity():
    t, s = iotas(BLOCK, BLOCK)
    return jnp.where(s == t, 1.0, 0.0).astype(F32)


def pieces(channels, repeats):
    found = []
    for start in range(0, channels, LANES):
        width = min(LANES, channels - start)
        heads = [start // HEAD_DIM + i for i in range(width // HEAD_DIM)]
        found.append((start, width, heads, heads[0] // repeats))
    return found


def spread(columns, heads, width):
    first = jnp.broadcast_to(columns[:, heads[0] : heads[0] + 1], (BLOCK, width))
    if len(heads) == 1:
        return first
    second = jnp.broadcast_to(columns[:, heads[1] : heads[1] + 1], (BLOCK, width))
    lane = iotas(BLOCK, width)[1]
    return jnp.where(lane < HEAD_DIM, first, second)


def state_kernel(
    repeats, at_ref, x_ref, b_ref, step_ref, log_ref, prefix_ref, base_ref, total_ref, all_ref, s_ref, l_ref
):
    k = pl.program_id(0)
    channels = x_ref.shape[1]

    @pl.when(k == 0)
    def _():
        s_ref[...] = jnp.zeros_like(s_ref)
        l_ref[...] = jnp.zeros_like(l_ref)

    columns = dot(lower_ones(), log_ref[...], 1, 1, HIGHEST)
    steps = dot(identity(), step_ref[...], 1, 1, HIGHEST)
    base_ref[0] = l_ref[...]
    prefix_ref[0] = s_ref[...].astype(BF16)
    for start, width, heads, group in pieces(channels, repeats):
        lanes = pl.ds(start, width)
        cum = spread(columns, heads, width)
        last = cum[BLOCK - 1 : BLOCK, :]
        weighted = (
            x_ref[:, lanes].astype(F32) * (jnp.exp(last - cum) * spread(steps, heads, width))
        ).astype(BF16)
        new = dot(b_ref[:, group * STATE : (group + 1) * STATE], weighted, 0, 0)
        s_ref[:, lanes] = jnp.exp(last) * s_ref[:, lanes] + new
        l_ref[:, lanes] = l_ref[:, lanes] + last
    total_ref[...] = s_ref[...]
    all_ref[...] = jnp.exp(l_ref[...])


def within_kernel(
    repeats, at_ref, x_ref, b_ref, c_ref, step_ref, log_ref, skip_ref, prefix_ref, y_ref
):
    channels = x_ref.shape[1]
    half = BLOCK // 2
    lower = lower_ones()
    columns = dot(lower, log_ref[...], 1, 1, HIGHEST)
    rows = dot(log_ref[...], lower, 1, 1, HIGHEST) - jnp.log(step_ref[...])
    scores = {}
    for start, width, heads, group in pieces(channels, repeats):
        lanes = pl.ds(start, width)
        c_here = c_ref[:, group * STATE : (group + 1) * STATE]
        if group not in scores:
            full = dot(c_here, b_ref[:, group * STATE : (group + 1) * STATE], 1, 1)
            scores[group] = full * lower
        x_here = x_ref[:, lanes]
        lane = iotas(BLOCK, width)[1]
        top, bottom = 0.0, 0.0
        for i, head in enumerate(heads):
            kept = (lane >= i * HEAD_DIM) & (lane < (i + 1) * HEAD_DIM)
            x_head = x_here if len(heads) == 1 else jnp.where(kept, x_here, jnp.zeros_like(x_here))
            column, row = columns[:, head : head + 1], rows[head : head + 1, :]
            w_top = scores[group][:half, :half] * jnp.exp(
                jnp.minimum(column[:half] - row[:, :half], 0.0)
            )
            w_bottom = scores[group][half:] * jnp.exp(jnp.minimum(column[half:] - row, 0.0))
            top = top + dot(w_top.astype(BF16), x_head[:half], 1, 0)
            bottom = bottom + dot(w_bottom.astype(BF16), x_head, 1, 0)
        across = jnp.exp(spread(columns, heads, width)) * dot(c_here, prefix_ref[0, :, lanes], 1, 0)
        rest = across + skip_ref[:, lanes] * x_here.astype(F32)
        y_ref[:half, lanes] = (top + rest[:half]).astype(BF16)
        y_ref[half:, lanes] = (bottom + rest[half:]).astype(BF16)


def finish_kernel(
    repeats, at_ref, y_ref, gate_ref, c_ref, log_ref, base_ref, in_ref, gain_ref, w_ref, out_ref, sq_ref, g_ref
):
    channels = y_ref.shape[1]
    columns = dot(lower_ones(), log_ref[...], 1, 1, HIGHEST)
    squares = jnp.zeros((8, BLOCK), F32)
    for start, width, heads, group in pieces(channels, repeats):
        lanes = pl.ds(start, width)
        grow = jnp.exp(spread(columns, heads, width) + base_ref[0, 0:1, lanes])
        across = grow * dot(c_ref[:, group * STATE : (group + 1) * STATE], in_ref[:, lanes], 1, 0)
        gate = gate_ref[:, lanes].astype(F32)
        gated = (y_ref[:, lanes].astype(F32) + across) * (gate / (1.0 + jnp.exp(-gate)))
        squares = squares + dot(jnp.ones((8, width), BF16), (gated * gated).astype(BF16), 1, 1)
        g_ref[:, lanes] = (gated * gain_ref[:, lanes]).astype(BF16)
    sq_ref[...] = squares
    model = w_ref.shape[1]
    tile = 512 if model % 512 == 0 else model
    for start in range(0, model, tile):
        out_ref[:, start : start + tile] = dot(
            g_ref[...], w_ref[:, start : start + tile], 1, 0
        ).astype(BF16)


def shifted(value, axis, steps):
    count = lax.axis_size(axis)
    return lax.ppermute(value, axis, [(source, source + steps) for source in range(count - steps)])


def body(
    ssm_input, gate_input, b_proj, c_proj, step_size, log_decay, skip_gain, norm_gain, out_weight
):
    tokens, channels = ssm_input.shape
    heads = step_size.shape[0]
    blocks = tokens // BLOCK
    model = out_weight.shape[1]
    per_group = HEAD_COUNT // GROUPS
    groups = max(1, heads // per_group)
    repeats = min(heads, per_group)
    head_index = lax.axis_index("head")
    at = (head_index * heads // per_group // groups).astype(jnp.int32).reshape(1)
    skip = jnp.repeat(skip_gain, HEAD_DIM)[None, :]
    gain = lax.dynamic_slice_in_dim(norm_gain, head_index * channels, channels)[None, :]
    params = pltpu.CompilerParams(
        dimension_semantics=("arbitrary",), vmem_limit_bytes=56 * 1024 * 1024
    )

    def rows_of(width):
        return pl.BlockSpec((BLOCK, width), lambda k, at: (k, 0))

    grouped = pl.BlockSpec((BLOCK, groups * STATE), lambda k, at: (k, at[0]))
    head_rows = pl.BlockSpec((heads, BLOCK), lambda k, at: (0, k))
    fixed = lambda r, c: pl.BlockSpec((r, c), lambda k, at: (0, 0))
    state_block = pl.BlockSpec((1, STATE, channels), lambda k, at: (k, 0, 0))

    prefix, base, total, decay = pl.pallas_call(
        functools.partial(state_kernel, repeats),
        grid_spec=pltpu.PrefetchScalarGridSpec(
            num_scalar_prefetch=1,
            grid=(blocks,),
            in_specs=[rows_of(channels), grouped, head_rows, head_rows],
            out_specs=[
                state_block,
                pl.BlockSpec((1, 8, channels), lambda k, at: (k, 0, 0)),
                fixed(STATE, channels),
                fixed(8, channels),
            ],
            scratch_shapes=[pltpu.VMEM((STATE, channels), F32), pltpu.VMEM((8, channels), F32)],
        ),
        out_shape=[
            jax.ShapeDtypeStruct((blocks, STATE, channels), BF16),
            jax.ShapeDtypeStruct((blocks, 8, channels), F32),
            jax.ShapeDtypeStruct((STATE, channels), F32),
            jax.ShapeDtypeStruct((8, channels), F32),
        ],
        compiler_params=params,
        name="block_states",
        cost_estimate=pl.CostEstimate(
            flops=2 * tokens * channels * STATE, bytes_accessed=tokens * channels * 4, transcendentals=0
        ),
    )(at, ssm_input, b_proj, step_size, log_decay)

    incoming = shifted(total.astype(BF16), "seq", 1)
    for _ in range(lax.axis_size("seq") - 2):
        incoming = shifted((decay[0:1] * incoming.astype(F32) + total).astype(BF16), "seq", 1)

    shares = lax.axis_size("head")
    per_share = tokens // shares
    chunks = max(1, per_share // BLOCK)
    steps = blocks // chunks
    parts, squares = [], []
    for chunk in range(chunks):
        pick = lambda d, chunk=chunk: d * chunks + chunk
        picked = lambda width, pick=pick: pl.BlockSpec((BLOCK, width), lambda d, at: (pick(d), 0))
        y = pl.pallas_call(
            functools.partial(within_kernel, repeats),
            grid_spec=pltpu.PrefetchScalarGridSpec(
                num_scalar_prefetch=1,
                grid=(steps,),
                in_specs=[
                    picked(channels),
                    pl.BlockSpec((BLOCK, groups * STATE), lambda d, at: (pick(d), at[0])),
                    pl.BlockSpec((BLOCK, groups * STATE), lambda d, at: (pick(d), at[0])),
                    pl.BlockSpec((heads, BLOCK), lambda d, at: (0, pick(d))),
                    pl.BlockSpec((heads, BLOCK), lambda d, at: (0, pick(d))),
                    fixed(1, channels),
                    pl.BlockSpec((1, STATE, channels), lambda d, at: (pick(d), 0, 0)),
                ],
                out_specs=rows_of(channels),
            ),
            out_shape=jax.ShapeDtypeStruct((steps * BLOCK, channels), BF16),
            compiler_params=params,
            name="within",
            cost_estimate=pl.CostEstimate(
                flops=16 * steps * BLOCK * channels * BLOCK, bytes_accessed=steps * BLOCK * channels * 8, transcendentals=0
            ),
        )(at, ssm_input, b_proj, c_proj, step_size, log_decay, skip, prefix)
        partial, square = pl.pallas_call(
            functools.partial(finish_kernel, repeats),
            grid_spec=pltpu.PrefetchScalarGridSpec(
                num_scalar_prefetch=1,
                grid=(steps,),
                in_specs=[
                    rows_of(channels),
                    picked(channels),
                    pl.BlockSpec((BLOCK, groups * STATE), lambda d, at: (pick(d), at[0])),
                    pl.BlockSpec((heads, BLOCK), lambda d, at: (0, pick(d))),
                    pl.BlockSpec((1, 8, channels), lambda d, at: (pick(d), 0, 0)),
                    fixed(STATE, channels),
                    fixed(1, channels),
                    fixed(channels, model),
                ],
                out_specs=[
                    pl.BlockSpec((BLOCK, model), lambda d, at: (d, 0)),
                    pl.BlockSpec((8, BLOCK), lambda d, at: (0, d)),
                ],
                scratch_shapes=[pltpu.VMEM((BLOCK, channels), BF16)],
            ),
            out_shape=[
                jax.ShapeDtypeStruct((steps * BLOCK, model), BF16),
                jax.ShapeDtypeStruct((8, steps * BLOCK), F32),
            ],
            compiler_params=params,
            name="finish",
            cost_estimate=pl.CostEstimate(
                flops=2 * steps * BLOCK * channels * model,
                bytes_accessed=steps * BLOCK * (channels * 4 + model * 2) + channels * model * 2,
                transcendentals=0,
            ),
        )(at, y, gate_input, c_proj, log_decay, base, incoming, gain, out_weight)
        parts.append(lax.psum_scatter(partial, "head", scatter_dimension=0, tiled=True))
        squares.append(square[0].reshape(shares, per_share // chunks))
    squares = lax.psum_scatter(
        jnp.concatenate(squares, axis=1), "head", scatter_dimension=0, tiled=True
    ).reshape(per_share, 1)
    scale = lax.rsqrt(squares / (HEAD_COUNT * HEAD_DIM) + epsilon)
    return (jnp.concatenate(parts, axis=0).astype(F32) * scale).astype(BF16)


def solution(mesh):
    in_specs = (
        P(("batch", "seq"), "head"),
        P(("batch", "seq"), "head"),
        P(("batch", "seq"), None),
        P(("batch", "seq"), None),
        P("head", ("batch", "seq")),
        P("head", ("batch", "seq")),
        P("head"),
        P(),
        P("head", None),
    )
    out_specs = P(("batch", "seq", "head"), None)
    return jax.shard_map(body, mesh=mesh, in_specs=in_specs, out_specs=out_specs, check_vma=False)
```
